16 devices in a mesh: rep: 1, dp: 16 (over x, y, z, core).
Axes of the slice: x: 2, y: 2, z: 2, core: 2. Of those that a mesh axis runs over, the one named last changes fastest.
Arguments:
- g_w_gate: bfloat16 [16, 2, 1152, 4608], P(('rep', 'dp'))
- g_w_up: bfloat16 [16, 2, 1152, 4608], P(('rep', 'dp'))
- g_w_down: bfloat16 [16, 2, 4608, 1152], P(('rep', 'dp'))
- w_gate: bfloat16 [2, 1152, 4608], replicated
- w_up: bfloat16 [2, 1152, 4608], replicated
- w_down: bfloat16 [2, 4608, 1152], replicated
- m_w_gate: float32 [2, 1152, 4608], P(None, 'dp')
- m_w_up: float32 [2, 1152, 4608], P(None, 'dp')
- m_w_down: float32 [2, 4608, 1152], P(None, 'dp')
- v_w_gate: float32 [2, 1152, 4608], P(None, 'dp')
- v_w_up: float32 [2, 1152, 4608], P(None, 'dp')
- v_w_down: float32 [2, 4608, 1152], P(None, 'dp')
Outputs:
- output 1: bfloat16 [2, 1152, 4608], P('rep')
- output 2: bfloat16 [2, 1152, 4608], P('rep')
- output 3: bfloat16 [2, 4608, 1152], P('rep')
- output 4: float32 [2, 1152, 4608], P('rep', 'dp')
- output 5: float32 [2, 1152, 4608], P('rep', 'dp')
- output 6: float32 [2, 4608, 1152], P('rep', 'dp')
- output 7: float32 [2, 1152, 4608], P('rep', 'dp')
- output 8: float32 [2, 1152, 4608], P('rep', 'dp')
- output 9: float32 [2, 4608, 1152], P('rep', 'dp')
All inputs are finite; a program needn't handle non-finite values.
Results may differ from the reference program's by a relative error of at most 0.022.
Values are sent between devices in bfloat16 or wider.
A program may use at most 2 GiB of HBM per device.

```python
import jax
import jax.numpy as jnp
from jax import lax

DEVICES = 16
D = 1152
FF = 4608
LAYERS = 2
NAMES = ("w_gate", "w_up", "w_down")
SHAPES = {"w_gate": (LAYERS, D, FF), "w_up": (LAYERS, D, FF), "w_down": (LAYERS, FF, D)}


def setup_inputs(seed: int = 0, part: int = 0) -> dict:
    kz, *keys = jax.random.split(jax.random.key(seed), 1 + 5 * len(NAMES))
    loud = 2.0 ** jax.random.uniform(kz, (), jnp.float32, -1.0, 1.0)
    drawn = {}
    for name, key, both in zip(NAMES, keys[:3], keys[3:6], strict=True):
        own = jax.random.normal(jax.random.fold_in(key, part), (DEVICES, *SHAPES[name]), jnp.float32)
        shared = jax.random.normal(jax.random.fold_in(both, part), SHAPES[name], jnp.float32)
        drawn["g_" + name] = (loud * (0.7 * shared / DEVICES + 0.7 * own * DEVICES**-0.5)).astype(jnp.bfloat16)
    for name, key in zip(NAMES, keys[6:9], strict=True):
        drawn[name] = (jax.random.normal(key, SHAPES[name], jnp.float32) * SHAPES[name][1] ** -0.5).astype(jnp.bfloat16)
    for name, key in zip(NAMES, keys[9:12], strict=True):
        drawn["m_" + name] = loud * 0.5 * jax.random.normal(key, SHAPES[name], jnp.float32)
    for name, key in zip(NAMES, keys[12:15], strict=True):
        drawn["v_" + name] = loud * loud * jax.random.uniform(key, SHAPES[name], jnp.float32, 0.5, 1.5)
    return drawn


def adamw(w, m, v, g):
    m = 0.9 * m + 0.1 * g
    v = 0.95 * v + 0.05 * g * g
    step = m * lax.rsqrt(v + 1e-8) + 0.1 * w
    return (w - 0.02 * step).astype(jnp.bfloat16), m, v


def clipped(gradients, sum_of_squares, count):
    factor = jnp.minimum(1.0, 0.5 * lax.rsqrt(sum_of_squares / count + 1e-30))
    return [g * factor for g in gradients]


def reference(g_w_gate, g_w_up, g_w_down, w_gate, w_up, w_down, m_w_gate, m_w_up, m_w_down, v_w_gate, v_w_up, v_w_down):
    def total(terms):
        return lax.scan(lambda so_far, term: (so_far + term.astype(jnp.float32), None), jnp.zeros(terms.shape[1:], jnp.float32), terms)[0]

    gradients = [total(terms).astype(jnp.bfloat16).astype(jnp.float32) for terms in (g_w_gate, g_w_up, g_w_down)]
    gradients = clipped(gradients, sum(jnp.sum(g * g) for g in gradients), sum(g.size for g in gradients))
    new = [
        adamw(w.astype(jnp.float32), m, v, g)
        for w, m, v, g in zip((w_gate, w_up, w_down), (m_w_gate, m_w_up, m_w_down), (v_w_gate, v_w_up, v_w_down), gradients, strict=True)
    ]
    return tuple(one[which] for which in range(3) for one in new)
```

```python
import functools

import jax
import jax.numpy as jnp
from jax import lax
from jax.experimental import pallas as pl
from jax.experimental.pallas import tpu as pltpu
from jax.sharding import PartitionSpec as P

MESH = pl.DeviceIdType.MESH
BF16, F32 = jnp.bfloat16, jnp.float32
DEVICES, CHIPS, COLOURS, LAYERS, WEIGHTS = 16, 8, 3, 2, 3
AXES = (4, 2, 1)
TILE = (8, 128)
STEP = 12


def tiles_of(a):
    layers, rows, columns = a.shape
    a = a.reshape(layers, rows // 8, 8, columns // 128, 128)
    return a.transpose(0, 1, 3, 2, 4).reshape(layers, rows * columns // 1024, 8, 128)


def rows_of(a, rows, columns):
    layers = a.shape[0]
    a = a.reshape(layers, rows // 8, columns // 128, 8, 128)
    return a.transpose(0, 1, 3, 2, 4).reshape(layers, rows, columns)


def flip(chip, q):
    out = chip
    for axis in AXES:
        if q & axis:
            out = out + axis * (1 - 2 * (chip // axis % 2))
    return out


def device(index):
    return {"dp": index}


def greet(others):
    barrier = pltpu.get_barrier_semaphore()
    for other in others:
        pl.semaphore_signal(barrier, inc=1, device_id=device(other), device_id_type=MESH)
    pl.semaphore_wait(barrier, len(others))


def axes_of(colour):
    return tuple(AXES[(colour + i) % 3] for i in range(3))


def scatter_kernel(per, *refs):
    terms, (out, squares, landed) = refs[:3], refs[3:6]
    own1, land1, own2, land2, own3, land3, own4, land4, got1, got2, got3, mine, theirs = refs[6:19]
    pair_send, pair_recv, load1, load2, load3, load4, send1, send2, send3, recv1, recv2, recv3, sq_send, sq_recv = refs[19:]
    me = lax.axis_index("dp")
    chip, core = me // 2, me % 2
    sibling = chip * 2 + 1 - core
    part = per // COLOURS
    triples = WEIGHTS * LAYERS
    greet([lax.rem(me + i, DEVICES) for i in range(1, DEVICES)])

    def pair_copy(w, layer, n, q):
        block = flip(chip, q) * 2 + 1 - core
        return pltpu.make_async_remote_copy(
            src_ref=terms[w].at[layer, pl.ds(block * per, per)],
            dst_ref=landed.at[w * LAYERS + layer, q],
            send_sem=pair_send.at[w * LAYERS + layer, n],
            recv_sem=pair_recv.at[w * LAYERS + layer, n],
            device_id=device(sibling),
            device_id_type=MESH,
        )

    order = (7, 3, 5, 6, 1, 2, 4, 0)
    for w in range(WEIGHTS):

        @pl.loop(0, LAYERS)
        def _(layer):
            for n, q in enumerate(order):
                pair_copy(w, layer, n, q).start()

    def units(stage):
        found = []
        for slot in range((4, 2, 1, 1)[stage - 1]):
            for colour in range(COLOURS):
                d1, d2, d3 = axes_of(colour)
                if stage == 1:
                    slot_ = 3 - slot
                    q = d1 + (slot_ // 2) * d2 + (slot_ % 2) * d3
                elif stage == 2:
                    slot_ = 1 - slot
                    q = d2 + slot_ * d3
                else:
                    slot_ = 0
                    q = d3 if stage == 3 else 0
                found.append((colour, slot_, q))
        return found

    stages = {1: (own1, land1, load1), 2: (own2, land2, load2), 3: (own3, land3, load3), 4: (own4, land4, load4)}

    def own_copy(stage, w, layer, colour, slot, q, at):
        own, _, sem = stages[stage]
        block = flip(chip, q) * 2 + core
        return pltpu.make_async_copy(
            terms[w].at[layer, pl.ds(block * per + colour * part, part)], own.at[at, colour, slot], sem.at[at, colour, slot, 0]
        )

    def land_copy(stage, t, colour, slot, q, at):
        _, land, sem = stages[stage]
        return pltpu.make_async_copy(
            landed.at[t, q, pl.ds(colour * part, part)], land.at[at, colour, slot], sem.at[at, colour, slot, 1]
        )

    def load(stage, t):
        at = t % 2
        for w in range(WEIGHTS):

            @pl.when(t // LAYERS == w)
            def _():
                for colour, slot, q in units(stage):
                    own_copy(stage, w, t % LAYERS, colour, slot, q, at).start()

        for colour, slot, q in units(stage):
            land_copy(stage, t, colour, slot, q, at).start()

    def wait_load(stage, t, colour, slot, q):
        own_copy(stage, 0, t % LAYERS, colour, slot, q, t % 2).wait()
        land_copy(stage, t, colour, slot, q, t % 2).wait()

    def send(stage, t, colour, slot):
        source = stages[stage][0]
        target, s_sem, r_sem = {1: (got1, send1, recv1), 2: (got2, send2, recv2), 3: (got3, send3, recv3)}[stage]
        other = flip(chip, axes_of(colour)[stage - 1]) * 2 + core
        return pltpu.make_async_remote_copy(
            src_ref=source.at[t % 2, colour, slot],
            dst_ref=target.at[t, colour, slot],
            send_sem=s_sem.at[t % 2, colour, slot],
            recv_sem=r_sem.at[t, colour, slot],
            device_id=device(other),
            device_id_type=MESH,
        )

    def add(t, stage, colour, slot):
        own, land, _ = stages[stage]
        at = t % 2
        sources = [own.at[at, colour, slot], land.at[at, colour, slot]]
        if stage == 2:
            sources.append(got1.at[t, colour, 2 + slot])
        if stage == 3:
            sources += [got1.at[t, colour, 1], got2.at[t, colour, 1]]
        if stage == 4:
            sources += [got1.at[t, colour, 0], got2.at[t, colour, 0], got3.at[t, colour, 0]]

        @pl.loop(0, part // STEP)
        def _(i):
            here = pl.ds(i * STEP, STEP)
            total = sources[0][here].astype(F32)
            for source in sources[1:]:
                total = total + source[here].astype(F32)
            rounded = total.astype(BF16)
            if stage < 4:
                sources[0][here] = rounded
            else:
                out[t, pl.ds(colour * part + i * STEP, STEP)] = rounded
                g = rounded.astype(F32)
                mine[...] += jnp.sum(g * g, axis=0)

    mine[...] = jnp.zeros_like(mine)

    def wait_pair(t):
        for n, q in enumerate(order):
            pltpu.make_async_remote_copy(
                src_ref=terms[0].at[0, pl.ds(0, per)],
                dst_ref=landed.at[t, q],
                send_sem=pair_send.at[t, n],
                recv_sem=pair_recv.at[t, n],
                device_id=device(sibling),
                device_id_type=MESH,
            ).wait()

    wait_pair(0)
    load(1, 0)

    @pl.loop(0, triples + 3)
    def _(t):
        @pl.when(t < triples)
        def _():
            for colour, slot, q in units(1):
                wait_load(1, t, colour, slot, q)
                add(t, 1, colour, slot)
                send(1, t, colour, slot).start()

            @pl.when(t + 1 < triples)
            def _():
                wait_pair(t + 1)

        @pl.when((t >= 1) & (t < triples + 1))
        def _():
            for colour, slot, q in units(2):
                wait_load(2, t - 1, colour, slot, q)
                send(1, t - 1, colour, 2 + slot).wait_recv()
                add(t - 1, 2, colour, slot)
                send(2, t - 1, colour, slot).start()

        @pl.when((t >= 2) & (t < triples + 2))
        def _():
            for colour, slot, q in units(3):
                wait_load(3, t - 2, colour, slot, q)
                send(1, t - 2, colour, 1).wait_recv()
                send(2, t - 2, colour, 1).wait_recv()
                add(t - 2, 3, colour, slot)
                send(3, t - 2, colour, slot).start()

        @pl.when(t >= 3)
        def _():
            for colour, slot, q in units(4):
                wait_load(4, t - 3, colour, slot, q)
                send(1, t - 3, colour, 0).wait_recv()
                send(2, t - 3, colour, 0).wait_recv()
                send(3, t - 3, colour, 0).wait_recv()
                add(t - 3, 4, colour, slot)
                send(3, t - 3, colour, 0).wait_send()

        @pl.when((t >= 2) & (t < triples + 2))
        def _():
            for colour, slot, q in units(2):
                send(2, t - 2, colour, slot).wait_send()

        @pl.when((t >= 1) & (t < triples + 1))
        def _():
            for colour, slot, q in units(1):
                send(1, t - 1, colour, slot).wait_send()

        @pl.when(t + 1 < triples)
        def _():
            load(1, t + 1)

        @pl.when(t < triples)
        def _():
            load(2, t)

        @pl.when((t >= 1) & (t < triples + 1))
        def _():
            load(3, t - 1)

        @pl.when((t >= 2) & (t < triples + 2))
        def _():
            load(4, t - 2)

    def tell(i):
        other = lax.rem(me + i, DEVICES)
        return pltpu.make_async_remote_copy(
            src_ref=mine,
            dst_ref=theirs.at[i],
            send_sem=sq_send.at[i],
            recv_sem=sq_recv.at[i],
            device_id=device(other),
            device_id_type=MESH,
        )

    for i in range(1, DEVICES):
        tell(i).start()
    for i in range(1, DEVICES):
        tell(i).wait()
    theirs[0] = mine[...]
    total = jnp.zeros(TILE, F32)
    for i in range(DEVICES):
        total = total + theirs[lax.rem(me - i + DEVICES, DEVICES)]
    squares[...] = total


def gather_kernel(per, *refs):
    blocks, whole, (held, hold_in, hold_out, send_sem, recv_sem, pair_send, pair_recv) = refs[:3], refs[3:6], refs[6:]
    me = lax.axis_index("dp")
    chip, core = me // 2, me % 2
    sibling = chip * 2 + 1 - core
    part = per // COLOURS
    greet([flip(chip, axis) * 2 + core for axis in AXES] + [sibling])

    def source(w, layer, colour, q):
        if q == 0:
            return blocks[w].at[layer, pl.ds(colour * part, part)]
        return place(w, layer, colour, q)

    def place(w, layer, colour, q):
        return whole[w].at[layer, pl.ds((flip(chip, q) * 2 + core) * per + colour * part, part)]

    def hop(w, layer, colour, stage, slot):
        d = axes_of(colour)
        q = (slot % 2) * d[0] + (slot // 2) * d[1]
        n = (0, 1, 3)[stage - 1] + slot
        t = w * LAYERS + layer
        return q, pltpu.make_async_remote_copy(
            src_ref=source(w, layer, colour, q),
            dst_ref=place(w, layer, colour, q),
            send_sem=send_sem.at[t, colour, n],
            recv_sem=recv_sem.at[t, colour, n],
            device_id=device(flip(chip, d[stage - 1]) * 2 + core),
            device_id_type=MESH,
        )

    def across(w, layer, colour, q):
        t = w * LAYERS + layer
        return pltpu.make_async_remote_copy(
            src_ref=source(w, layer, colour, q),
            dst_ref=place(w, layer, colour, q),
            send_sem=pair_send.at[t, colour, q],
            recv_sem=pair_recv.at[t, colour, q],
            device_id=device(sibling),
            device_id_type=MESH,
        )

    def over_all(body):
        for w in range(WEIGHTS):

            @pl.loop(0, LAYERS)
            def _(layer):
                for colour in range(COLOURS):
                    body(w, layer, colour)

    def own_in(w):
        return pltpu.make_async_copy(blocks[w], held.at[w], hold_in.at[w])

    def own_out(w):
        return pltpu.make_async_copy(held.at[w], whole[w].at[:, pl.ds(me * per, per)], hold_out.at[w])

    over_all(lambda w, layer, colour: hop(w, layer, colour, 1, 0)[1].start())
    over_all(lambda w, layer, colour: hop(w, layer, colour, 2, 0)[1].start())
    over_all(lambda w, layer, colour: hop(w, layer, colour, 3, 0)[1].start())
    over_all(lambda w, layer, colour: across(w, layer, colour, 0).start())
    for w in range(WEIGHTS):
        own_in(w).start()
    for w in range(WEIGHTS):
        own_in(w).wait()
        own_out(w).start()

    def after_first(w, layer, colour):
        d1, d2, d3 = axes_of(colour)
        hop(w, layer, colour, 1, 0)[1].wait_recv()
        hop(w, layer, colour, 2, 1)[1].start()
        across(w, layer, colour, d1).start()

    def after_second(w, layer, colour):
        d1, d2, d3 = axes_of(colour)
        hop(w, layer, colour, 3, 1)[1].start()
        for slot in range(2):
            hop(w, layer, colour, 2, slot)[1].wait_recv()
            hop(w, layer, colour, 3, 2 + slot)[1].start()
            across(w, layer, colour, d2 + slot * d1).start()

    def after_third(w, layer, colour):
        d1, d2, d3 = axes_of(colour)
        for slot in range(4):
            hop(w, layer, colour, 3, slot)[1].wait_recv()
            across(w, layer, colour, d3 + (slot % 2) * d1 + (slot // 2) * d2).start()

    over_all(after_first)
    over_all(after_second)
    over_all(after_third)

    def finish(w, layer, colour):
        for stage in (1, 2, 3):
            for slot in range((1, 2, 4)[stage - 1]):
                hop(w, layer, colour, stage, slot)[1].wait_send()
        for q in range(CHIPS):
            across(w, layer, colour, q).wait()

    over_all(finish)
    for w in range(WEIGHTS):
        own_out(w).wait()


def adamw(w, m, v, g):
    m = 0.9 * m + 0.1 * g
    v = 0.95 * v + 0.05 * g * g
    step = m * lax.rsqrt(v + 1e-8) + 0.1 * w
    return (w - 0.02 * step).astype(BF16), m, v


def solution(mesh):
    any_space = pl.BlockSpec(memory_space=pl.ANY)
    vmem = pl.BlockSpec(memory_space=pltpu.VMEM)
    dma = pltpu.SemaphoreType.DMA

    def scatter(terms):
        per = terms[0].shape[1] // DEVICES
        part = per // COLOURS
        triples = WEIGHTS * LAYERS
        unit = (part, *TILE)

        def buffers(slots):
            return [pltpu.VMEM((2, COLOURS, slots, *unit), BF16)] * 2

        return pl.pallas_call(
            functools.partial(scatter_kernel, per),
            out_shape=[
                jax.ShapeDtypeStruct((triples, per, *TILE), BF16),
                jax.ShapeDtypeStruct(TILE, F32),
                jax.ShapeDtypeStruct((triples, CHIPS, per, *TILE), BF16),
            ],
            in_specs=[any_space] * 3,
            out_specs=[vmem, vmem, any_space],
            scratch_shapes=[
                *buffers(4), *buffers(2), *buffers(1), *buffers(1),
                pltpu.VMEM((triples, COLOURS, 4, *unit), BF16),
                pltpu.VMEM((triples, COLOURS, 2, *unit), BF16),
                pltpu.VMEM((triples, COLOURS, 1, *unit), BF16),
                pltpu.VMEM(TILE, F32),
                pltpu.VMEM((DEVICES, *TILE), F32),
                dma((triples, CHIPS)), dma((triples, CHIPS)),
                dma((2, COLOURS, 4, 2)), dma((2, COLOURS, 2, 2)), dma((2, COLOURS, 1, 2)), dma((2, COLOURS, 1, 2)),
                dma((2, COLOURS, 4)), dma((2, COLOURS, 2)), dma((2, COLOURS, 1)),
                dma((triples, COLOURS, 4)), dma((triples, COLOURS, 2)), dma((triples, COLOURS, 1)),
                dma((DEVICES,)), dma((DEVICES,)),
            ],
            compiler_params=pltpu.CompilerParams(collective_id=0, has_side_effects=True, vmem_limit_bytes=62 * 2**20),
            name="reduce_scatter",
        )(*terms)

    def gather(blocks):
        layers, per = blocks[0].shape[:2]
        triples = WEIGHTS * LAYERS
        return pl.pallas_call(
            functools.partial(gather_kernel, per),
            out_shape=[jax.ShapeDtypeStruct((layers, per * DEVICES, *TILE), BF16)] * 3,
            in_specs=[any_space] * 3,
            out_specs=[any_space] * 3,
            scratch_shapes=[
                pltpu.VMEM((WEIGHTS, layers, per, *TILE), BF16),
                dma((WEIGHTS,)), dma((WEIGHTS,)),
                dma((triples, COLOURS, 7)), dma((triples, COLOURS, 7)),
                dma((triples, COLOURS, CHIPS)), dma((triples, COLOURS, CHIPS)),
            ],
            compiler_params=pltpu.CompilerParams(collective_id=1, has_side_effects=True),
            name="all_gather",
        )(*blocks)

    def step(*arrays):
        terms, weights, m, v = (arrays[i : i + 3] for i in (0, 3, 6, 9))
        sizes = [one.shape[1:] for one in m]
        sums, squares, _ = scatter([tiles_of(t[0]) for t in terms])
        sums, squares, m, v = lax.optimization_barrier((sums, squares, m, v))
        count = DEVICES * sum(one.size for one in m)
        factor = jnp.minimum(1.0, 0.5 * lax.rsqrt(jnp.sum(squares) / count + 1e-30))
        me = lax.axis_index("dp")
        new = []
        for i in range(WEIGHTS):
            per = sums.shape[1]
            own = lax.dynamic_slice_in_dim(tiles_of(weights[i]), me * per, per, 1).astype(F32)
            g = sums[i * LAYERS : (i + 1) * LAYERS].astype(F32) * factor
            new.append(adamw(own, tiles_of(m[i]), tiles_of(v[i]), g))
        whole = gather([one[0] for one in new])
        return (
            *(rows_of(one, *w.shape[1:]) for one, w in zip(whole, weights, strict=True)),
            *(rows_of(one[1], *size) for one, size in zip(new, sizes, strict=True)),
            *(rows_of(one[2], *size) for one, size in zip(new, sizes, strict=True)),
        )

    all_of, cut = P(None, None, None), P(None, "dp", None)
    return jax.shard_map(
        step,
        mesh=mesh,
        in_specs=(P(("rep", "dp"), None, None, None),) * 3 + (all_of,) * 3 + (cut,) * 6,
        out_specs=(P("rep", None, None),) * 3 + (P("rep", "dp", None),) * 6,
        check_vma=False,
    )
```

```python
import functools

import jax
import jax.numpy as jnp
from jax import lax
from jax.experimental import pallas as pl
from jax.experimental.pallas import tpu as pltpu
from jax.sharding import PartitionSpec as P


MESH = pl.DeviceIdType.MESH
BF16, F32 = jnp.bfloat16, jnp.float32
DEVICES, CHIPS, COLOURS, LAYERS, WEIGHTS = 16, 8, 3, 2, 3
AXES = (4, 2, 1)
TILE = (8, 128)
STEP = 12
LATE = ((1, 1), (2, 0), (2, 1))


def tiles_of(a):
    layers, rows, columns = a.shape
    a = a.reshape(layers, rows // 8, 8, columns // 128, 128)
    return a.transpose(0, 1, 3, 2, 4).reshape(layers, rows * columns // 1024, 8, 128)


def rows_of(a, rows, columns):
    layers = a.shape[0]
    a = a.reshape(layers, rows // 8, columns // 128, 8, 128)
    return a.transpose(0, 1, 3, 2, 4).reshape(layers, rows, columns)


def flip(chip, q):
    out = chip
    for axis in AXES:
        if q & axis:
            out = out + axis * (1 - 2 * (chip // axis % 2))
    return out


def device(index):
    return {"dp": index}


def greet(others):
    barrier = pltpu.get_barrier_semaphore()
    for other in others:
        pl.semaphore_signal(barrier, inc=1, device_id=device(other), device_id_type=MESH)
    pl.semaphore_wait(barrier, len(others))


def axes_of(colour):
    return tuple(AXES[(colour + i) % 3] for i in range(3))


def scatter_kernel(per, *refs):
    terms, (out, squares, landed) = refs[:3], refs[3:6]
    own1, land1, own2, land2, own3, land3, own4, land4, got1, got2, got3, mine, theirs = refs[6:19]
    pair_send, pair_recv, load1, load2, load3, load4, send1, send2, send3, recv1, recv2, recv3, sq_send, sq_recv = refs[19:]
    me = lax.axis_index("dp")
    chip, core = me // 2, me % 2
    sibling = chip * 2 + 1 - core
    part = per // COLOURS
    triples = WEIGHTS * LAYERS

    order = (7, 3, 5, 6, 1, 2, 4, 0)

    def pair_copy(w, layer, n, q):
        block = flip(chip, q) * 2 + 1 - core
        return pltpu.make_async_remote_copy(
            src_ref=terms[w].at[layer, pl.ds(block * per, per)],
            dst_ref=landed.at[w * LAYERS + layer, q],
            send_sem=pair_send.at[w * LAYERS + layer, n],
            recv_sem=pair_recv.at[w * LAYERS + layer, n],
            device_id=device(sibling),
            device_id_type=MESH,
        )

    def units(stage):
        found = []
        for slot in range((4, 2, 1, 1)[stage - 1]):
            for colour in range(COLOURS):
                d1, d2, d3 = axes_of(colour)
                if stage == 1:
                    slot_ = 3 - slot
                    q = d1 + (slot_ // 2) * d2 + (slot_ % 2) * d3
                elif stage == 2:
                    slot_ = 1 - slot
                    q = d2 + slot_ * d3
                else:
                    slot_ = 0
                    q = d3 if stage == 3 else 0
                found.append((colour, slot_, q))
        return found

    stages = {1: (own1, land1, load1), 2: (own2, land2, load2), 3: (own3, land3, load3), 4: (own4, land4, load4)}

    def own_copy(stage, w, layer, colour, slot, q, at):
        own, _, sem = stages[stage]
        block = flip(chip, q) * 2 + core
        return pltpu.make_async_copy(
            terms[w].at[layer, pl.ds(block * per + colour * part, part)], own.at[at, colour, slot], sem.at[at, colour, slot, 0]
        )

    def land_copy(stage, t, colour, slot, q, at):
        _, land, sem = stages[stage]
        return pltpu.make_async_copy(
            landed.at[t, q, pl.ds(colour * part, part)], land.at[at, colour, slot], sem.at[at, colour, slot, 1]
        )

    def load(stage, t):
        at = t % 2
        for w in range(WEIGHTS):

            @pl.when(t // LAYERS == w)
            def _():
                for colour, slot, q in units(stage):
                    own_copy(stage, w, t % LAYERS, colour, slot, q, at).start()

        for colour, slot, q in units(stage):
            land_copy(stage, t, colour, slot, q, at).start()

    def wait_load(stage, t, colour, slot, q):
        own_copy(stage, 0, t % LAYERS, colour, slot, q, t % 2).wait()
        land_copy(stage, t, colour, slot, q, t % 2).wait()

    def send(stage, t, colour, slot):
        source = stages[stage][0]
        target, s_sem, r_sem = {1: (got1, send1, recv1), 2: (got2, send2, recv2), 3: (got3, send3, recv3)}[stage]
        other = flip(chip, axes_of(colour)[stage - 1]) * 2 + core
        return pltpu.make_async_remote_copy(
            src_ref=source.at[t % 2, colour, slot],
            dst_ref=target.at[t, colour, slot],
            send_sem=s_sem.at[t % 2, colour, slot],
            recv_sem=r_sem.at[t, colour, slot],
            device_id=device(other),
            device_id_type=MESH,
        )

    def add(t, stage, colour, slot):
        own, land, _ = stages[stage]
        at = t % 2
        sources = [own.at[at, colour, slot], land.at[at, colour, slot]]
        if stage == 2:
            sources.append(got1.at[t, colour, 2 + slot])
        if stage == 3:
            sources += [got1.at[t, colour, 1], got2.at[t, colour, 1]]
        if stage == 4:
            sources += [got1.at[t, colour, 0], got2.at[t, colour, 0], got3.at[t, colour, 0]]

        @pl.loop(0, part // STEP)
        def _(i):
            here = pl.ds(i * STEP, STEP)
            total = sources[0][here].astype(F32)
            for source in sources[1:]:
                total = total + source[here].astype(F32)
            rounded = total.astype(BF16)
            if stage < 4:
                sources[0][here] = rounded
            else:
                out[t, pl.ds(colour * part + i * STEP, STEP)] = rounded
                g = rounded.astype(F32)
                mine[...] += jnp.sum(g * g, axis=0)

    for colour, slot, q in units(1):
        own_copy(1, 0, 0, colour, slot, q, 0).start()
    greet([lax.rem(me + i, DEVICES) for i in range(1, DEVICES)])
    for w in range(WEIGHTS):

        @pl.loop(0, LAYERS)
        def _(layer):
            for n, q in enumerate(order):
                pair_copy(w, layer, n, q).start()

    mine[...] = jnp.zeros_like(mine)

    def pair_wait(t, n, q):
        return pltpu.make_async_remote_copy(
            src_ref=terms[0].at[0, pl.ds(0, per)],
            dst_ref=landed.at[t, q],
            send_sem=pair_send.at[t, n],
            recv_sem=pair_recv.at[t, n],
            device_id=device(sibling),
            device_id_type=MESH,
        )

    arrived = set()
    groups = [units(1)[i : i + COLOURS] for i in range(0, 4 * COLOURS, COLOURS)]
    for i in range(5):
        if i < 4:
            for n, q in enumerate(order):
                if q in [one[2] for one in groups[i]] and q not in arrived:
                    arrived.add(q)
                    pair_wait(0, n, q).wait_recv()
            for colour, slot, q in groups[i]:
                land_copy(1, 0, colour, slot, q, 0).start()
        if i > 0:
            for colour, slot, q in groups[i - 1]:
                wait_load(1, 0, colour, slot, q)
                add(0, 1, colour, slot)
                send(1, 0, colour, slot).start()
    for n, q in enumerate(order):
        if q not in arrived:
            pair_wait(0, n, q).wait_recv()

    @pl.loop(0, triples + 3)
    def _(t):
        @pl.when((t > 0) & (t < triples))
        def _():
            for colour, slot, q in units(1):
                wait_load(1, t, colour, slot, q)
                add(t, 1, colour, slot)
                send(1, t, colour, slot).start()

        @pl.when((t >= 1) & (t < triples + 1))
        def _():
            for colour, slot, q in units(2):
                wait_load(2, t - 1, colour, slot, q)
                send(1, t - 1, colour, 2 + slot).wait_recv()
                add(t - 1, 2, colour, slot)
                send(2, t - 1, colour, slot).start()

        @pl.when((t >= 2) & (t < triples + 2))
        def _():
            for colour, slot, q in units(3):
                wait_load(3, t - 2, colour, slot, q)
                send(1, t - 2, colour, 1).wait_recv()
                send(2, t - 2, colour, 1).wait_recv()
                add(t - 2, 3, colour, slot)
                send(3, t - 2, colour, slot).start()

        @pl.when(t >= 3)
        def _():
            for colour, slot, q in units(4):
                wait_load(4, t - 3, colour, slot, q)
                send(1, t - 3, colour, 0).wait_recv()
                send(2, t - 3, colour, 0).wait_recv()
                send(3, t - 3, colour, 0).wait_recv()
                add(t - 3, 4, colour, slot)
                send(3, t - 3, colour, 0).wait_send()

        @pl.when((t >= 2) & (t < triples + 2))
        def _():
            for colour, slot, q in units(2):
                send(2, t - 2, colour, slot).wait_send()

        @pl.when((t >= 1) & (t < triples + 1))
        def _():
            for colour, slot, q in units(1):
                send(1, t - 1, colour, slot).wait_send()

        @pl.when(t + 1 < triples)
        def _():
            for n, q in enumerate(order):
                pair_wait(t + 1, n, q).wait_recv()
            load(1, t + 1)

        @pl.when(t < triples)
        def _():
            load(2, t)

        @pl.when((t >= 1) & (t < triples + 1))
        def _():
            load(3, t - 1)

        @pl.when((t >= 2) & (t < triples + 2))
        def _():
            load(4, t - 2)

    def tell(i):
        other = lax.rem(me + i, DEVICES)
        return pltpu.make_async_remote_copy(
            src_ref=mine,
            dst_ref=theirs.at[i],
            send_sem=sq_send.at[i],
            recv_sem=sq_recv.at[i],
            device_id=device(other),
            device_id_type=MESH,
        )

    for i in range(1, DEVICES):
        tell(i).start()

    @pl.loop(0, triples)
    def _(t):
        for n, q in enumerate(order):
            pair_wait(t, n, q).wait_send()

    for i in range(1, DEVICES):
        tell(i).wait()
    theirs[0] = mine[...]
    total = jnp.zeros(TILE, F32)
    for i in range(DEVICES):
        total = total + theirs[lax.rem(me - i + DEVICES, DEVICES)]
    squares[...] = total


def adamw(w, m, v, g):
    m = 0.9 * m + 0.1 * g
    v = 0.95 * v + 0.05 * g * g
    step = m * lax.rsqrt(v + 1e-8) + 0.1 * w
    return (w - 0.02 * step).astype(BF16), m, v


def gather_kernel(per, *refs):
    sums, squares, weights, m_in, v_in = refs[0], refs[1], refs[2:5], refs[5:8], refs[8:11]
    whole, near, twin, m_out, v_out = refs[11:13], refs[13:19], refs[19], refs[20], refs[21]
    g_held, w_held, m_held, v_held, new, load_sem, store_sem, near_sem, send_sem, recv_sem, pair_send, pair_recv = refs[22:]
    me = lax.axis_index("dp")
    chip, core = me // 2, me % 2
    sibling = chip * 2 + 1 - core
    part = per // COLOURS

    def loads(w, layer):
        t = w * LAYERS + layer
        return [
            pltpu.make_async_copy(sums.at[t], g_held.at[t], load_sem.at[t, 0]),
            pltpu.make_async_copy(m_in[w].at[layer], m_held.at[t], load_sem.at[t, 1]),
            pltpu.make_async_copy(v_in[w].at[layer], v_held.at[t], load_sem.at[t, 2]),
            pltpu.make_async_copy(weights[w].at[layer, pl.ds(me * per, per)], w_held.at[t], load_sem.at[t, 3]),
        ]

    def slot_of(colour, q):
        d1, d2, _ = axes_of(colour)
        return (1 if q & d1 else 0) + (2 if q & d2 else 0)

    def late_slot(w, layer, colour, q):
        i = LATE.index((w, layer))
        return near[i // 2 * COLOURS + colour].at[i % 2 * 4 + slot_of(colour, q)]

    def place(w, layer, colour, q):
        if w > 0 and (w, layer) in LATE:
            return late_slot(w, layer, colour, q)
        return whole[w].at[layer, pl.ds((flip(chip, q) * 2 + core) * per + colour * part, part)]

    def source(w, layer, colour, q):
        if q == 0:
            return new.at[w * LAYERS + layer, pl.ds(colour * part, part)]
        return place(w, layer, colour, q)

    def hop(w, layer, colour, stage, slot):
        d = axes_of(colour)
        q = (slot % 2) * d[0] + (slot // 2) * d[1]
        n = (0, 1, 3)[stage - 1] + slot
        t = w * LAYERS + layer
        if w > 0 and (w, layer) in LATE:
            target = late_slot(w, layer, colour, q + d[stage - 1])
        else:
            target = place(w, layer, colour, q)
        return pltpu.make_async_remote_copy(
            src_ref=source(w, layer, colour, q),
            dst_ref=target,
            send_sem=send_sem.at[t, colour, n],
            recv_sem=recv_sem.at[t, colour, n],
            device_id=device(flip(chip, d[stage - 1]) * 2 + core),
            device_id_type=MESH,
        )

    def across(w, layer, colour, q):
        t = w * LAYERS + layer
        if w > 0 and (w, layer) in LATE:
            target = twin.at[LATE.index((w, layer)), colour, slot_of(colour, q)]
        else:
            target = place(w, layer, colour, q)
        return pltpu.make_async_remote_copy(
            src_ref=source(w, layer, colour, q),
            dst_ref=target,
            send_sem=pair_send.at[t, colour, q],
            recv_sem=pair_recv.at[t, colour, q],
            device_id=device(sibling),
            device_id_type=MESH,
        )

    def each(body, late=True):
        @pl.loop(0, LAYERS)
        def _(layer):
            body(0, layer)

        body(1, 0)
        if late:
            for w, layer in LATE:
                body(w, layer)

    def over_all(body, late=True):
        each(lambda w, layer: [body(w, layer, colour) for colour in range(COLOURS)], late)

    def stores(w, layer):
        t = w * LAYERS + layer
        found = [
            pltpu.make_async_copy(m_held.at[t], m_out.at[t], store_sem.at[t, 0]),
            pltpu.make_async_copy(v_held.at[t], v_out.at[t], store_sem.at[t, 1]),
        ]
        if w > 0 and (w, layer) in LATE:
            for colour in range(COLOURS):
                found.append(
                    pltpu.make_async_copy(
                        new.at[t, pl.ds(colour * part, part)], place(w, layer, colour, 0), near_sem.at[LATE.index((w, layer)), colour]
                    )
                )
        else:
            found.append(pltpu.make_async_copy(new.at[t], whole[w].at[layer, pl.ds(me * per, per)], store_sem.at[t, 2]))
        return found

    def fetch(w, layer):
        for one in loads(w, layer):
            one.start()

    fetch(0, 0)
    fetch(0, 1)
    greet([flip(chip, axis) * 2 + core for axis in AXES] + [sibling])
    count = WEIGHTS * LAYERS * per * DEVICES * 1024
    factor = jnp.minimum(1.0, 0.5 * lax.rsqrt(jnp.sum(squares[...]) / count + 1e-30))

    def compute(w, layer):
        t = w * LAYERS + layer
        for one in loads(w, layer):
            one.wait()
        if w == 0:

            @pl.when(layer == 0)
            def _():
                fetch(1, 0)

            @pl.when(layer == 1)
            def _():
                fetch(1, 1)
        elif w == 1:
            fetch(2, layer)
        for colour in range(COLOURS):

            @pl.loop(0, part // STEP)
            def _(i):
                here = pl.ds(colour * part + i * STEP, STEP)
                g = g_held[t, here].astype(F32) * factor
                new[t, here], m_held[t, here], v_held[t, here] = adamw(w_held[t, here].astype(F32), m_held[t, here], v_held[t, here], g)

            hop(w, layer, colour, 1, 0).start()
        for one in stores(w, layer):
            one.start()

    each(compute)
    over_all(lambda w, layer, colour: hop(w, layer, colour, 2, 0).start())
    over_all(lambda w, layer, colour: across(w, layer, colour, 0).start())

    def after_first(w, layer, colour):
        hop(w, layer, colour, 1, 0).wait_recv()
        hop(w, layer, colour, 2, 1).start()
        across(w, layer, colour, axes_of(colour)[0]).start()

    def after_second(w, layer, colour):
        d1, d2, _ = axes_of(colour)
        for slot in range(2):
            hop(w, layer, colour, 2, slot).wait_recv()
            across(w, layer, colour, d2 + slot * d1).start()
            if w == 0 or (w, layer) not in LATE:
                hop(w, layer, colour, 3, 2 + slot).start()

    def after_third(w, layer, colour):
        d1, d2, d3 = axes_of(colour)
        for slot in range(4):
            hop(w, layer, colour, 3, slot).wait_recv()
            across(w, layer, colour, d3 + (slot % 2) * d1 + (slot // 2) * d2).start()

    def third_early(w, layer, colour):
        hop(w, layer, colour, 3, 0).start()
        hop(w, layer, colour, 3, 1).start()

    over_all(after_first)
    over_all(third_early, late=False)
    over_all(after_second)
    over_all(after_third, late=False)

    def finish(w, layer, colour):
        early = w == 0 or (w, layer) not in LATE
        for stage in (1, 2, 3)[: 3 if early else 2]:
            for slot in range((1, 2, 4)[stage - 1]):
                hop(w, layer, colour, stage, slot).wait_send()
        d1, d2, d3 = axes_of(colour)
        for q in (0, d1, d2, d1 + d2, d3, d3 + d1, d3 + d2, 7)[: 8 if early else 4]:
            across(w, layer, colour, q).wait()

    over_all(finish)
    each(lambda w, layer: [one.wait() for one in stores(w, layer)])


def copy_all(jobs, slots):
    def drain(job):
        source, stores_, buffer, load_sem, store_sem = job
        pltpu.make_async_copy(source, buffer, load_sem).wait()
        for i, (piece, target) in enumerate(stores_):
            pltpu.make_async_copy(piece, target, store_sem.at[i]).start()

    def settle(job):
        _, stores_, _, _, store_sem = job
        for i, (piece, target) in enumerate(stores_):
            pltpu.make_async_copy(piece, target, store_sem.at[i]).wait()

    ahead = slots // 2
    for i in range(len(jobs) + ahead):
        if i < len(jobs):
            if i >= slots:
                settle(jobs[i - slots])
            pltpu.make_async_copy(jobs[i][0], jobs[i][2], jobs[i][3]).start()
        if i >= ahead:
            drain(jobs[i - ahead])
    for job in jobs[max(0, len(jobs) - slots) :]:
        settle(job)


COPY_SLOTS = 12


def copy_whole(per, source, target, layers, slots, load_sem, store_sem):
    piece = 2 * per
    jobs = []
    for layer in range(layers):
        for i in range(DEVICES // 2):
            s = len(jobs) % COPY_SLOTS
            here = pl.ds(i * piece, piece)
            jobs.append((source.at[layer, here], [(slots.at[s], target.at[layer, here])], slots.at[s], load_sem.at[s], store_sem.at[s]))
    return jobs


def near_jobs(per, near, twin, target, layer, quads, load_sem, store_sem, first):
    me = lax.axis_index("dp")
    jobs = []
    for colour in range(COLOURS):
        for other in range(2):
            s = (first + len(jobs)) % COPY_SLOTS
            source = twin.at[colour] if other else near[colour]
            jobs.append((source, quarters(per, me, target, layer, colour, other, 0, quads.at[s]), quads.at[s], load_sem.at[s], store_sem.at[s]))
    return jobs


def gate_kernel(per, source, target, slots, load_sem, store_sem):
    copy_all(copy_whole(per, source, target, LAYERS, slots, load_sem, store_sem), COPY_SLOTS)


def up_kernel(per, source, *refs):
    near, twin, target, slots, quads, load_sem, store_sem = refs[:3], refs[3], *refs[4:]
    jobs = copy_whole(per, source, target, 1, slots, load_sem, store_sem)
    jobs += near_jobs(per, [one.at[pl.ds(0, 4)] for one in near], twin.at[0], target, 1, quads, load_sem, store_sem, len(jobs))
    copy_all(jobs, COPY_SLOTS)


def rest_kernel(per, *refs):
    m_in, v_in, near, twin, outs, down = refs[0], refs[1], refs[2:8], refs[8], refs[9:15], refs[15]
    slots, quads, load_sem, store_sem = refs[16:]
    jobs = []
    for w in range(WEIGHTS):
        for layer in range(LAYERS):
            for source, target in ((m_in, outs[w]), (v_in, outs[3 + w])):
                s = len(jobs) % COPY_SLOTS
                jobs.append(
                    (source.at[w * LAYERS + layer], [(slots.at[s], target.at[layer])], slots.at[s], load_sem.at[s], store_sem.at[s])
                )
    for layer in range(LAYERS):
        mine = near[COLOURS:] if layer else [one.at[pl.ds(4, 4)] for one in near[:COLOURS]]
        jobs += near_jobs(per, mine, twin.at[1 + layer], down, layer, quads, load_sem, store_sem, len(jobs))
    copy_all(jobs, COPY_SLOTS)


def quarters(per, me, down, layer, colour, other, last, buffer):
    d1, d2, d3 = axes_of(colour)
    chip, core = me // 2, me % 2
    if other:
        core = 1 - core
    part = per // COLOURS
    found = []
    for slot in range(4):
        q = (slot % 2) * d1 + (slot // 2) * d2 + last * d3
        found.append((buffer.at[slot], down.at[layer, pl.ds((flip(chip, q) * 2 + core) * per + colour * part, part)]))
    return found


def far_kernel(per, parts, n, *refs):
    far, outs, sem = refs[n : n + 2 * COLOURS], refs[n + 2 * COLOURS : 2 * n + 2 * COLOURS], refs[-1]
    me = lax.axis_index("dp")
    copies = []
    for which, layer, first in parts:
        for other in range(2):
            for colour in range(COLOURS):
                source = far[other * COLOURS + colour].at[pl.ds(first, 4)]
                for slot, (piece, target) in enumerate(quarters(per, me, outs[which], layer, colour, other, 1, source)):
                    copies.append(pltpu.make_async_copy(piece, target, sem.at[which, other, colour, slot]))
    for one in copies:
        one.start()
    for one in copies:
        one.wait()


def solution(mesh):
    any_space = pl.BlockSpec(memory_space=pl.ANY)
    vmem = pl.BlockSpec(memory_space=pltpu.VMEM)
    dma = pltpu.SemaphoreType.DMA

    def scatter(terms):
        per = terms[0].shape[1] // DEVICES
        part = per // COLOURS
        triples = WEIGHTS * LAYERS
        unit = (part, *TILE)

        def buffers(slots):
            return [pltpu.VMEM((2, COLOURS, slots, *unit), BF16)] * 2

        return pl.pallas_call(
            functools.partial(scatter_kernel, per),
            out_shape=[
                jax.ShapeDtypeStruct((triples, per, *TILE), BF16),
                jax.ShapeDtypeStruct(TILE, F32),
                jax.ShapeDtypeStruct((triples, CHIPS, per, *TILE), BF16),
            ],
            in_specs=[any_space] * 3,
            out_specs=[vmem, vmem, any_space],
            scratch_shapes=[
                *buffers(4), *buffers(2), *buffers(1), *buffers(1),
                pltpu.VMEM((triples, COLOURS, 4, *unit), BF16),
                pltpu.VMEM((triples, COLOURS, 2, *unit), BF16),
                pltpu.VMEM((triples, COLOURS, 1, *unit), BF16),
                pltpu.VMEM(TILE, F32),
                pltpu.VMEM((DEVICES, *TILE), F32),
                dma((triples, CHIPS)), dma((triples, CHIPS)),
                dma((2, COLOURS, 4, 2)), dma((2, COLOURS, 2, 2)), dma((2, COLOURS, 1, 2)), dma((2, COLOURS, 1, 2)),
                dma((2, COLOURS, 4)), dma((2, COLOURS, 2)), dma((2, COLOURS, 1)),
                dma((triples, COLOURS, 4)), dma((triples, COLOURS, 2)), dma((triples, COLOURS, 1)),
                dma((DEVICES,)), dma((DEVICES,)),
            ],
            compiler_params=pltpu.CompilerParams(collective_id=0, has_side_effects=True, vmem_limit_bytes=62 * 2**20),
            name="reduce_scatter",
        )(*terms)

    def gather(sums, squares, weights, m, v):
        triples, per = sums.shape[:2]
        unit = (per // COLOURS, *TILE)
        full = jax.ShapeDtypeStruct((LAYERS, per * DEVICES, *TILE), BF16)
        quad = jax.ShapeDtypeStruct((4, *unit), BF16)
        moment = jax.ShapeDtypeStruct((triples, per, *TILE), F32)
        return pl.pallas_call(
            functools.partial(gather_kernel, per),
            out_shape=[
                full,
                jax.ShapeDtypeStruct((1, *full.shape[1:]), BF16),
                *[jax.ShapeDtypeStruct((8, *unit), BF16)] * COLOURS,
                *[quad] * COLOURS,
                jax.ShapeDtypeStruct((len(LATE), COLOURS, 4, *unit), BF16),
                moment,
                moment,
            ],
            in_specs=[any_space, vmem] + [any_space] * 9,
            out_specs=[any_space] * (5 + 2 * COLOURS),
            scratch_shapes=[
                pltpu.VMEM((triples, per, *TILE), BF16),
                pltpu.VMEM((triples, per, *TILE), BF16),
                pltpu.VMEM((triples, per, *TILE), F32),
                pltpu.VMEM((triples, per, *TILE), F32),
                pltpu.VMEM((triples, per, *TILE), BF16),
                dma((triples, 4)), dma((triples, 3)), dma((len(LATE), COLOURS)),
                dma((triples, COLOURS, 7)), dma((triples, COLOURS, 7)),
                dma((triples, COLOURS, CHIPS)), dma((triples, COLOURS, CHIPS)),
            ],
            compiler_params=pltpu.CompilerParams(collective_id=1, has_side_effects=True),
            name="all_gather",
        )(sums, squares, *weights, *m, *v)

    def settle(kernel, scratch, out_shape, *given):
        size = sum(one.size * one.dtype.itemsize for one in given)
        return pl.pallas_call(
            kernel,
            out_shape=out_shape,
            in_specs=[any_space] * len(given),
            out_specs=jax.tree.map(lambda _: any_space, out_shape),
            scratch_shapes=[*scratch, dma((COPY_SLOTS,)), dma((COPY_SLOTS, 4))],
            cost_estimate=pl.CostEstimate(flops=2 * 10**8, bytes_accessed=2 * size, transcendentals=0),
        )(*given)

    def settle_far(parts, outs, far):
        n = len(outs)
        per = outs[0].shape[1] // DEVICES
        size = sum(2 * one.size for one in far)
        return pl.pallas_call(
            functools.partial(far_kernel, per, parts, n),
            out_shape=[jax.ShapeDtypeStruct(one.shape, BF16) for one in outs],
            in_specs=[any_space] * n + [vmem] * len(far),
            out_specs=[any_space] * n,
            scratch_shapes=[dma((n, 2, COLOURS, 4))],
            input_output_aliases={i: i for i in range(n)},
            cost_estimate=pl.CostEstimate(flops=10**7, bytes_accessed=2 * size, transcendentals=0),
            compiler_params=pltpu.CompilerParams(vmem_limit_bytes=size + 2**21),
            name="settle_far",
        )(*outs, *far)

    def swap(one, bit):
        return lax.ppermute(one, "dp", [(i, i + bit * (1 - 2 * (i // bit % 2))) for i in range(DEVICES)])

    def whole_step(*arrays):
        terms, weights, m, v = (arrays[i : i + 3] for i in (0, 3, 6, 9))
        sizes = [one.shape[1:] for one in m]
        sums, squares, _ = scatter([tiles_of(t[0]) for t in terms])
        got = gather(sums, squares, *([tiles_of(one) for one in kind] for kind in (weights, m, v)))
        gate, up, near, twin, m_new, v_new = *got[:2], got[2:8], *got[8:]
        far = []
        for i in range(2):
            for c in range(COLOURS):
                far.append(swap(near[i * COLOURS + c], 2 * axes_of(c)[2]))
        per = sums.shape[1]
        full = jax.ShapeDtypeStruct(gate.shape, BF16)
        moment = jax.ShapeDtypeStruct((LAYERS, per, *TILE), F32)
        pairs_of = pltpu.VMEM((COPY_SLOTS, 2 * per, *TILE), BF16)
        floats = pltpu.VMEM((COPY_SLOTS, per, *TILE), F32)
        quads = pltpu.VMEM((COPY_SLOTS, 4, per // COLOURS, *TILE), BF16)
        gate = settle(functools.partial(gate_kernel, per), [pairs_of], full, gate)
        up = settle(functools.partial(up_kernel, per), [pairs_of, quads], full, up, *near[:COLOURS], twin)
        *moments, down = settle(
            functools.partial(rest_kernel, per), [floats, quads], [moment] * 6 + [full], m_new, v_new, *near, twin
        )
        twins = []
        for i in range(2):
            for c in range(COLOURS):
                twins.append(swap(far[i * COLOURS + c], 1))
        up, down = settle_far(((0, 1, 0), (1, 0, 4)), [up, down], far[:COLOURS] + twins[:COLOURS])
        (down,) = settle_far(((0, 1, 0),), [down], far[COLOURS:] + twins[COLOURS:])
        results = [gate, up, down]
        return (
            *(rows_of(one, *w.shape[1:]) for one, w in zip(results, weights, strict=True)),
            *(rows_of(one, *size) for one, size in zip(moments, sizes * 2, strict=True)),
        )

    all_of, cut = P(None, None, None), P(None, "dp", None)

    return jax.shard_map(
        whole_step,
        mesh=mesh,
        in_specs=(P(("rep", "dp"), None, None, None),) * 3 + (all_of,) * 3 + (cut,) * 6,
        out_specs=(P("rep", None, None),) * 3 + (P("rep", "dp", None),) * 6,
        check_vma=False,
    )
```
